32 devices in a mesh: groups: 2 (over x), tp: 8 (over z, y), blk: 2 (over core).
Axes of the slice: x: 2, y: 2, z: 4, core: 2. Of those that a mesh axis runs over, the one named last changes fastest.
Arguments:
- tokens: bfloat16 [4096, 7168], P(('groups', 'tp')), parts along dimension 0, may hold values from -6 to 6
- gate_weight: bfloat16 [7168, 2048], P('tp', 'blk'), may hold values from -0.0625 to 0.0625
- up_weight: bfloat16 [7168, 2048], P('tp', 'blk'), may hold values from -0.0625 to 0.0625
- down_weight: bfloat16 [2048, 7168], P('blk', 'tp'), may hold values from -0.125 to 0.125
Outputs:
- mixed: bfloat16 [4096, 7168], P(('groups', 'blk'), 'tp'), parts along dimension 0
The draws below stay inside these ranges and needn't reach their ends.
There are 2 independent parts, one for each index of `groups`. The reference program is written for one: setup_inputs(seed, part) draws one part's arguments, and reference() takes and returns one part's arrays. A program takes and returns all parts, laid end to end along the dimension named above; an argument that names none is the same for every part. Nothing has to cross between parts.
All inputs are finite; a program needn't handle non-finite values.
Results may differ from the reference program's by a relative error of at most 0.005.
Values may be sent and summed in bfloat16 or wider, within the bound.
A program may use at most 128 MiB of HBM per device.

```python
import jax
import jax.numpy as jnp

D = 7168
FF = 2048
TOKENS = 2048


def shard_levels(key, extent, shards, least, top_value):
    gain, own = 1.0, jax.random.fold_in(key, 6)
    for position, blocks in shards:
        heights = jnp.exp(jax.random.uniform(jax.random.fold_in(own, position), (blocks,), jnp.float32, least / len(shards), top_value / len(shards)))
        gain = gain * jnp.repeat(heights, extent[position] // blocks).reshape([-1 if axis == position else 1 for axis in range(len(extent))])
    return gain


def bell_draw(stream_key, shape, spread, bound, cuts=(), dtype=jnp.bfloat16):
    factor_of = shard_levels(stream_key, shape, cuts, -0.22, 0.18) if cuts else 1.0
    array = jax.random.normal(stream_key, shape, jnp.float32) * spread * factor_of
    return jnp.minimum(jnp.maximum(array, -bound), bound).astype(dtype)


def setup_inputs(seed: int = 0, part: int = 0) -> dict:
    key_list = jax.random.split(jax.random.key(seed), 5)
    own_keys = jax.random.split(jax.random.fold_in(key_list[4], part), 5)
    tokens = bell_draw(own_keys[0], (TOKENS, D), 1.0, 6.0, ((0, 8),))
    gate_weight = bell_draw(key_list[1], (D, FF), D ** -0.5, 0.0625, ((0, 8), (1, 2)))
    up_weight = bell_draw(key_list[2], (D, FF), D ** -0.5, 0.0625, ((0, 8), (1, 2)))
    down_weight = bell_draw(key_list[3], (FF, D), FF ** -0.5, 0.125, ((0, 2), (1, 8)))
    return dict(tokens=tokens, gate_weight=gate_weight, up_weight=up_weight, down_weight=down_weight)


def reference(tokens, gate_weight, up_weight, down_weight):
    gate = jnp.dot(tokens, gate_weight, preferred_element_type=jnp.float32)
    up = jnp.dot(tokens, up_weight, preferred_element_type=jnp.float32)
    hidden = (jax.nn.silu(gate) * up).astype(jnp.bfloat16)
    return jnp.dot(hidden, down_weight, preferred_element_type=jnp.float32).astype(jnp.bfloat16)
```

```python
import functools

import jax
import jax.numpy as jnp
from jax import lax
from jax.experimental import pallas as pl
from jax.experimental.pallas import tpu as pltpu
from jax.sharding import PartitionSpec as P

MESH = pl.DeviceIdType.MESH
ANY = pl.BlockSpec(memory_space=pl.ANY)


def flip1(i):
    return i + 1 - 2 * (i % 2)


def greet(devices):
    barrier = pltpu.get_barrier_semaphore()
    for device in devices:
        pl.semaphore_signal(barrier, inc=1, device_id=device, device_id_type=MESH)
    pl.semaphore_wait(barrier, len(devices))


def exchange(
    G, n, B,
    tok, gate, up, down, T, W, D,
    v_tok, v_w, v_down,
    lsem, tok_send, tok_recv, core_send, core_recv,
    w_send, w_recv, x_send, x_recv, d_send, d_recv,
):
    g, t, b = lax.axis_index("groups"), lax.axis_index("tp"), lax.axis_index("blk")
    h = n // B
    a, j = t // h, t % h
    other = (g, t, 1 - b)
    width = tok.shape[1] // B
    depth, units = gate.shape[0], gate.shape[1] // h
    part = depth // G
    mine = pl.ds(pl.multiple_of(b * width, 128), width)

    greet(
        [(g, (t + d) % n, b) for d in range(1, n)]
        + [((g + e) % G, t, b) for e in range(1, G)]
        + [other]
    )

    def remote(src, dst, send, recv, device):
        return pltpu.make_async_remote_copy(
            src_ref=src, dst_ref=dst, send_sem=send, recv_sem=recv,
            device_id=device, device_id_type=MESH,
        )

    def local(src, dst, sem):
        return pltpu.make_async_copy(src, dst, sem)

    def token_block(slot):
        return T.at[slot, :, mine]

    own_columns = pl.ds(pl.multiple_of(j * units, 128), units)
    loads = [
        local(tok, v_tok, lsem.at[0]),
        local(gate.at[:, own_columns], v_w.at[:, pl.ds(0, units)], lsem.at[1]),
        local(up.at[:, own_columns], v_w.at[:, pl.ds(units, units)], lsem.at[2]),
        local(down, v_down, lsem.at[3]),
    ]
    for load in loads:
        load.start()

    square = h == 4
    if square:
        def flip2(i):
            return i + 2 - 4 * (i // 2)

        near = [flip1(j), flip2(j)]
        sources = near + [flip1(flip2(j))]
        direct = 2
    else:
        near = [(j + d) % h for d in range(1, h)]
        sources = [(j - d + h) % h for d in range(1, h)]
        direct = h - 1
    pending = []
    for k in range(direct):
        c = remote(tok.at[:, mine], token_block(j), tok_send.at[k], tok_recv.at[k], (g, a * h + near[k], b))
        c.start()
        pending.append(c)

    rows = pl.ds(pl.multiple_of(g * part, 16), part)

    order = [n // 2] + [d for k in range(1, n // 2) for d in (n // 2 - k, n // 2 + k)]

    def weight_copy(d, k):
        src = (gate, up)[k]
        dest = (t + d) % n
        cols = pl.ds(pl.multiple_of((dest % h) * units, 128), units)
        return remote(
            src.at[rows, cols], W.at[t, rows, pl.ds(k * units, units)],
            w_send.at[d, k], w_recv.at[d, k], (g, dest, b),
        )

    for d in order:
        for k in range(2):
            c = weight_copy(d, k)
            c.start()
            pending.append(c)

    c = remote(down, D.at[b], d_send, d_recv, other)
    c.start()
    pending.append(c)

    for load in loads:
        load.wait()
    stores = [
        local(v_tok, T.at[j], lsem.at[0]),
        local(v_w, W.at[t], lsem.at[1]),
        local(v_down, D.at[b], lsem.at[3]),
    ]
    for store in stores:
        store.start()

    def to_other(k):
        block = token_block(sources[k])
        c = remote(block, block, core_send.at[k], core_recv.at[k], other)
        c.start()
        pending.append(c)

    def arrived(k):
        block = token_block(sources[k])
        remote(block, block, tok_send.at[k], tok_recv.at[k], other).wait_recv()

    if square:
        arrived(0)
        arrived(1)
        passed = j + 1 - 2 * (j % 2) + b * (flip2(j) - flip1(j))
        target = flip2(j) + b * (flip1(j) - flip2(j))
        block = token_block(passed)
        c = remote(block, block, tok_send.at[2], tok_recv.at[2], (g, a * h + target, b))
        c.start()
        pending.append(c)
        to_other(0)
        to_other(1)
    else:
        for k in range(h - 1):
            arrived(k)
            to_other(k)

    for d in order:
        source = (t - d + n) % n
        for k in range(2):
            block = W.at[source, rows, pl.ds(k * units, units)]
            remote(block, block, w_send.at[d, k], w_recv.at[d, k], other).wait_recv()
            for e in range(1, G):
                c = remote(block, block, x_send.at[e, d, k], x_recv.at[e, d, k], ((g + e) % G, t, b))
                c.start()
                pending.append(c)
    if square:
        arrived(2)
        to_other(2)

    theirs = pl.ds(pl.multiple_of((1 - b) * width, 128), width)
    for k in range(h - 1):
        block = T.at[sources[k], :, theirs]
        remote(block, block, core_send.at[k], core_recv.at[k], other).wait_recv()
    for d in order:
        source = (t - d + n) % n
        for e in range(1, G):
            their_rows = pl.ds(pl.multiple_of(((g - e + G) % G) * part, 16), part)
            for k in range(2):
                block = W.at[source, their_rows, pl.ds(k * units, units)]
                remote(block, block, x_send.at[e, d, k], x_recv.at[e, d, k], other).wait_recv()
    remote(D.at[1 - b], D.at[1 - b], d_send, d_recv, other).wait_recv()
    for c in pending:
        c.wait_send()
    for store in stores:
        store.wait()


def spread(n, B, hid, H, v_hid, lsem, send, recv, f_send, f_recv):
    g, t, b = lax.axis_index("groups"), lax.axis_index("tp"), lax.axis_index("blk")
    h = n // B
    a = t // h
    half, pairs = h // 2, n // 2
    p, y = t // 2, t % 2
    units = hid.shape[1]
    other = (g, t, 1 - b)
    across = (g, flip1(t), b)

    greet(
        [(g, (2 * ((p + d) % pairs) + y), c) for d in range(1, pairs) for c in range(B)]
        + [other, across]
    )

    def remote(src, dst, s, r, device):
        return pltpu.make_async_remote_copy(
            src_ref=src, dst_ref=dst, send_sem=s, recv_sem=r,
            device_id=device, device_id_type=MESH,
        )

    def columns(k, yy, c):
        return pl.ds(pl.multiple_of((c * h + 2 * k + yy) * units, 128), units)

    own = p % half
    place = H.at[:, columns(own, y, b)]
    load = pltpu.make_async_copy(hid, v_hid, lsem)
    load.start()
    copies = []
    for d in sorted(range(1, pairs), key=lambda d: -min(d, pairs - d)):
        c = remote(hid, place, send.at[d], recv.at[own, b], (g, 2 * ((p + d) % pairs) + y, a))
        c.start()
        copies.append(c)
    load.wait()

    @pl.when(a == b)
    def _():
        pltpu.make_async_copy(v_hid, place, recv.at[own, b]).start()

    @pl.when(a != b)
    def _():
        c = remote(hid, place, send.at[0], recv.at[own, b], other)
        c.start()
        c.wait_send()

    for k in range(half):
        for c in range(B):
            block = H.at[:, columns(k, y, c)]
            remote(block, block, send.at[0], recv.at[k, c], other).wait_recv()
            f = remote(block, block, f_send.at[k, c], f_recv.at[k, c], across)
            f.start()
            copies.append(f)
    for k in range(half):
        for c in range(B):
            block = H.at[:, columns(k, 1 - y, c)]
            remote(block, block, f_send.at[k, c], f_recv.at[k, c], across).wait_recv()
    for c in copies:
        c.wait_send()


def local(G, n, B, tokens, gate_weight, up_weight, down_weight):
    h = n // B
    R, K = tokens.shape
    depth, wide = gate_weight.shape
    units = wide // h
    dtype = tokens.dtype
    DMA = pltpu.SemaphoreType.DMA
    T, W, D = pl.pallas_call(
        functools.partial(exchange, G, n, B),
        out_shape=[
            jax.ShapeDtypeStruct((h, R, K), dtype),
            jax.ShapeDtypeStruct((n, depth, 2 * units), dtype),
            jax.ShapeDtypeStruct((B,) + down_weight.shape, dtype),
        ],
        in_specs=[ANY] * 4,
        out_specs=[ANY] * 3,
        scratch_shapes=[
            pltpu.VMEM((R, K), dtype),
            pltpu.VMEM((depth, 2 * units), dtype),
            pltpu.VMEM(down_weight.shape, dtype),
            DMA((4,)),
            DMA((h,)), DMA((h,)), DMA((h,)), DMA((h,)),
            DMA((n, 2)), DMA((n, 2)),
            DMA((G, n, 2)), DMA((G, n, 2)),
            DMA, DMA,
        ],
        compiler_params=pltpu.CompilerParams(collective_id=0, has_side_effects=True),
        name="exchange",
    )(tokens, gate_weight, up_weight, down_weight)
    both = jnp.dot(
        T.reshape(h * R, K), W.reshape(n * depth, 2 * units),
        preferred_element_type=jnp.float32,
    )
    hidden = (jax.nn.silu(both[:, :units]) * both[:, units:]).astype(dtype)
    half = h // 2
    H = pl.pallas_call(
        functools.partial(spread, n, B),
        out_shape=jax.ShapeDtypeStruct((h * R, B * wide), dtype),
        in_specs=[ANY],
        out_specs=ANY,
        scratch_shapes=[
            pltpu.VMEM((h * R, units), dtype),
            DMA,
            DMA((n // 2,)), DMA((half, B)), DMA((half, B)), DMA((half, B)),
        ],
        compiler_params=pltpu.CompilerParams(collective_id=1, has_side_effects=True),
        name="spread",
    )(hidden)
    result = jnp.dot(H, D.reshape(B * down_weight.shape[0], -1), preferred_element_type=jnp.float32)
    return result.astype(dtype)


def solution(mesh):
    shape = dict(mesh.shape)
    return jax.shard_map(
        functools.partial(local, shape["groups"], shape["tp"], shape["blk"]),
        mesh=mesh,
        in_specs=(P(("groups", "tp"), None), P("tp", "blk"), P("tp", "blk"), P("blk", "tp")),
        out_specs=P(("groups", "blk"), "tp"),
        check_vma=False,
    )
```

```python
import functools

import jax
import jax.numpy as jnp
from jax import lax
from jax.experimental import pallas as pl
from jax.experimental.pallas import tpu as pltpu
from jax.sharding import PartitionSpec as P

MESH = pl.DeviceIdType.MESH
ANY = pl.BlockSpec(memory_space=pl.ANY)


def flip1(i):
    return i + 1 - 2 * (i % 2)


def greet(devices):
    barrier = pltpu.get_barrier_semaphore()
    for device in devices:
        pl.semaphore_signal(barrier, inc=1, device_id=device, device_id_type=MESH)
    pl.semaphore_wait(barrier, len(devices))


def flip2(i):
    return i + 2 - 4 * ((i // 2) % 2)


def layer(
    G, n, B,
    tok, gate, up, down, out,
    T, W, D, both, mine_h, H, total,
    lsem, tok_send, tok_recv, core_send, core_recv,
    w_send, w_recv, x_send, x_recv, d_send, d_recv,
    h_send, h_recv, f_send, f_recv,
):
    g, t, b = lax.axis_index("groups"), lax.axis_index("tp"), lax.axis_index("blk")
    h = n // B
    a, j = t // h, t % h
    half, pairs = h // 2, n // 2
    p, y = t // 2, t % 2
    other = (g, t, 1 - b)
    across = (g, flip1(t), a * 0 + b)
    R, K = tok.shape
    width = K // B
    depth, units = gate.shape[0], gate.shape[1] // h
    part = depth // G
    mine = pl.ds(pl.multiple_of(b * width, 128), width)
    theirs = pl.ds(pl.multiple_of((1 - b) * width, 128), width)
    square = h == 4

    greet(
        [(g, (t + d) % n, b) for d in range(1, n)]
        + [(g, 2 * ((p + d) % pairs) + y, 1 - b) for d in range(1, pairs)]
        + [((g + e) % G, t, b) for e in range(1, G)]
        + [other]
    )

    def remote(src, dst, send, recv, device):
        return pltpu.make_async_remote_copy(
            src_ref=src, dst_ref=dst, send_sem=send, recv_sem=recv,
            device_id=device, device_id_type=MESH,
        )

    pending = []

    def push(*copy):
        c = remote(*copy)
        c.start()
        pending.append(c)

    def local(src, dst, sem):
        return pltpu.make_async_copy(src, dst, sem)

    def rows_of(i, s):
        if square:
            i = flip1(i) if s % 2 else i
            return flip2(i) if s // 2 else i
        return (i + h - s) % h

    def token_block(s):
        return T.at[rows_of(j, s), :, mine]

    def w_block(source, first, size, k):
        start = pl.multiple_of(source * depth + first, 16)
        return W.at[pl.ds(start, size), pl.ds(k * units, units)]

    own_columns = pl.ds(pl.multiple_of(j * units, 128), units)
    loads = [
        local(gate.at[:, own_columns], w_block(t, 0, depth, 0), lsem.at[0]),
        local(up.at[:, own_columns], w_block(t, 0, depth, 1), lsem.at[1]),
        local(tok, T.at[j], lsem.at[2]),
        local(down, D.at[b], lsem.at[3]),
    ]

    first = g * part
    rows = pl.ds(pl.multiple_of(first, 16), part)
    order = [n // 2] + [d for k in range(1, n // 2) for d in (n // 2 - k, n // 2 + k)]
    for d in order:
        dest = (t + d) % n
        cols = pl.ds(pl.multiple_of((dest % h) * units, 128), units)
        for k in range(2):
            push(
                (gate, up)[k].at[rows, cols], w_block(t, first, part, k),
                w_send.at[d, k], w_recv.at[d, k], (g, dest, b),
            )

    for s in (2, 1) if square else range(1, h):
        dest = rows_of(j, s) if square else (j + s) % h
        push(tok.at[:, mine], T.at[j, :, mine], tok_send.at[s], tok_recv.at[s], (g, a * h + dest, b))
    push(down, D.at[b], d_send, d_recv, other)
    for load in loads:
        load.start()

    for d in order:
        source = (t + n - d) % n
        for k in range(2):
            block = w_block(source, first, part, k)
            remote(block, block, w_send.at[d, k], w_recv.at[d, k], other).wait_recv()
            for e in range(1, G):
                push(block, block, x_send.at[e, d, k], x_recv.at[e, d, k], ((g + e) % G, t, b))
    for load in loads:
        load.wait()
    remote(D.at[1 - b], D.at[1 - b], d_send, d_recv, other).wait_recv()
    total[...] = jnp.zeros_like(total)

    def tokens_arrive(s):
        block = token_block(s)
        remote(block, block, tok_send.at[s], tok_recv.at[s], other).wait_recv()
        if square and s < 3:
            @pl.when(b == s - 1)
            def _():
                target = flip2(j) if s == 1 else flip1(j)
                remote(block, block, tok_send.at[3], tok_recv.at[3], (g, a * h + target, b)).start()

        push(block, block, core_send.at[s], core_recv.at[s], other)

    def compute(s):
        slot = rows_of(j, s)
        if s > 0:
            block = T.at[slot, :, theirs]
            remote(block, block, core_send.at[s], core_recv.at[s], other).wait_recv()
        tiles = 4 if K % 512 == 0 else 1
        tile = K // tiles
        both[...] = jnp.zeros_like(both)

        def body(i, carry):
            k = pl.ds(pl.multiple_of(i * tile, 128), tile)
            both[...] += jnp.dot(T[slot, :, k], W[k, :], preferred_element_type=jnp.float32)
            return carry

        lax.fori_loop(0, tiles, body, 0)
        hidden = (jax.nn.silu(both[:, :units]) * both[:, units:]).astype(out.dtype)
        mine_h[s] = hidden

        @pl.when(a == b)
        def _():
            H[s, j, b] = hidden

        for d in sorted(range(1, pairs), key=lambda d: -min(d, pairs - d)):
            push(
                mine_h.at[s], H.at[s, j, b], h_send.at[s, d], h_recv.at[s, j // 2, b],
                (g, 2 * ((p + d) % pairs) + y, a),
            )

        @pl.when(a != b)
        def _():
            remote(mine_h.at[s], H.at[s, j, b], h_send.at[s, 0], h_recv.at[s, j // 2, b], other).start()

    def pass_on(s):
        for k in range(half):
            for c in range(B):
                block = H.at[s, 2 * k + y, c]

                @pl.when(jnp.logical_not((a == b) & (j // 2 == k) & (c == b)))
                def _():
                    remote(block, block, h_send.at[s, 0], h_recv.at[s, k, c], other).wait_recv()

                push(block, block, f_send.at[s, k, c], f_recv.at[s, k, c], across)

    def lower(s):
        for k in range(half):
            for c in range(B):
                block = H.at[s, 2 * k + 1 - y, c]
                remote(block, block, f_send.at[s, k, c], f_recv.at[s, k, c], across).wait_recv()

        def body(i, carry):
            r = rows_of(i, s)
            term = total[r]
            for c in range(B):
                term += jnp.dot(
                    H[s, i, c], D[c, pl.ds(pl.multiple_of(i * units, 128), units), :],
                    preferred_element_type=jnp.float32,
                )
            total[r] = term
            return carry

        lax.fori_loop(0, h, body, 0)

    for d in order:
        source = (t + n - d) % n
        for e in range(1, G):
            for k in range(2):
                block = w_block(source, ((g + G - e) % G) * part, part, k)
                remote(block, block, x_send.at[e, d, k], x_recv.at[e, d, k], other).wait_recv()

    compute(0)
    for s in range(1, h):
        tokens_arrive(s)
        compute(s)
        pass_on(s - 1)
        if s >= 2:
            lower(s - 2)
    pass_on(h - 1)
    lower(h - 2)
    lower(h - 1)
    for r in range(h):
        out[pl.ds(r * R, R), :] = total[r].astype(out.dtype)

    for c in pending:
        c.wait_send()
    if square:
        remote(token_block(1), token_block(1), tok_send.at[3], tok_recv.at[3], other).wait_send()

    @pl.when(a != b)
    def _():
        for s in range(h):
            remote(mine_h.at[s], mine_h.at[s], h_send.at[s, 0], h_recv.at[s, 0, 0], other).wait_send()


def local(G, n, B, tokens, gate_weight, up_weight, down_weight):
    h = n // B
    R, K = tokens.shape
    depth, wide = gate_weight.shape
    units, columns = wide // h, down_weight.shape[1]
    dtype = tokens.dtype
    DMA = pltpu.SemaphoreType.DMA
    return pl.pallas_call(
        functools.partial(layer, G, n, B),
        out_shape=jax.ShapeDtypeStruct((h * R, columns), dtype),
        in_specs=[ANY] * 4,
        out_specs=pl.BlockSpec(memory_space=pltpu.VMEM),
        scratch_shapes=[
            pltpu.VMEM((h, R, K), dtype),
            pltpu.VMEM((K, 2 * units), dtype),
            pltpu.VMEM((B, wide, columns), dtype),
            pltpu.VMEM((R, 2 * units), jnp.float32),
            pltpu.VMEM((h, R, units), dtype),
            pltpu.VMEM((h, h, B, R, units), dtype),
            pltpu.VMEM((h, R, columns), jnp.float32),
            DMA((4,)),
            DMA((h,)), DMA((h,)), DMA((h,)), DMA((h,)),
            DMA((n, 2)), DMA((n, 2)),
            DMA((G, n, 2)), DMA((G, n, 2)),
            DMA, DMA,
            DMA((h, n // 2)), DMA((h, h // 2, B)),
            DMA((h, h // 2, B)), DMA((h, h // 2, B)),
        ],
        compiler_params=pltpu.CompilerParams(
            collective_id=0, has_side_effects=True, vmem_limit_bytes=63_000_000
        ),
        name="layer",
    )(tokens, gate_weight, up_weight, down_weight)


def solution(mesh):
    shape = dict(mesh.shape)
    return jax.shard_map(
        functools.partial(local, shape["groups"], shape["tp"], shape["blk"]),
        mesh=mesh,
        in_specs=(P(("groups", "tp"), None), P("tp", "blk"), P("tp", "blk"), P("blk", "tp")),
        out_specs=P(("groups", "blk"), "tp"),
        check_vma=False,
    )
```

```python
import functools

import jax
import jax.numpy as jnp
from jax import lax
from jax.experimental import pallas as pl
from jax.experimental.pallas import tpu as pltpu
from jax.sharding import PartitionSpec as P

MESH = pl.DeviceIdType.MESH
ANY = pl.BlockSpec(memory_space=pl.ANY)


def flip1(i):
    return i + 1 - 2 * (i % 2)


def greet(devices):
    barrier = pltpu.get_barrier_semaphore()
    for device in devices:
        pl.semaphore_signal(barrier, inc=1, device_id=device, device_id_type=MESH)
    pl.semaphore_wait(barrier, len(devices))


def flip2(i):
    return i + 2 - 4 * ((i // 2) % 2)


def layer(
    G, n, B,
    tok, gate, up, down, out,
    T, W, D, both, mine_h, H, total,
    lsem, tok_send, tok_recv, core_send, core_recv,
    w_send, w_recv, x_send, x_recv, d_send, d_recv,
    h_send, h_recv, f_send, f_recv,
):
    g, t, b = lax.axis_index("groups"), lax.axis_index("tp"), lax.axis_index("blk")
    h = n // B
    a, j = t // h, t % h
    half, pairs = h // 2, n // 2
    p, y = t // 2, t % 2
    other = (g, t, 1 - b)
    across = (g, flip1(t), b)
    R, K = tok.shape
    width = K // B
    depth, units = gate.shape[0], gate.shape[1] // h
    part = depth // G
    mine = pl.ds(pl.multiple_of(b * width, 128), width)
    theirs = pl.ds(pl.multiple_of((1 - b) * width, 128), width)
    square = h == 4

    greet(
        [(g, (t + d) % n, b) for d in range(1, n)]
        + [(g, 2 * ((p + d) % pairs) + y, 1 - b) for d in range(1, pairs)]
        + [((g + e) % G, t, b) for e in range(1, G)]
        + [other]
    )

    def remote(src, dst, send, recv, device):
        return pltpu.make_async_remote_copy(
            src_ref=src, dst_ref=dst, send_sem=send, recv_sem=recv,
            device_id=device, device_id_type=MESH,
        )

    pending = []

    def push(*copy):
        c = remote(*copy)
        c.start()
        pending.append(c)

    def local(src, dst, sem):
        return pltpu.make_async_copy(src, dst, sem)

    def rows_of(i, s):
        if square:
            i = flip1(i) if s % 2 else i
            return flip2(i) if s // 2 else i
        return (i + h - s) % h

    def token_block(s):
        return T.at[rows_of(j, s), :, mine]

    def w_block(source, first, size, k):
        start = pl.multiple_of(source * depth + first, 16)
        return W.at[pl.ds(start, size), pl.ds(k * units, units)]

    own_columns = pl.ds(pl.multiple_of(j * units, 128), units)
    loads = [
        local(gate.at[:, own_columns], w_block(t, 0, depth, 0), lsem.at[0]),
        local(up.at[:, own_columns], w_block(t, 0, depth, 1), lsem.at[1]),
        local(tok, T.at[j], lsem.at[2]),
        local(down, D.at[b], lsem.at[3]),
    ]

    first = g * part
    rows = pl.ds(pl.multiple_of(first, 16), part)
    order = [d for k in range(1, n // 2) for d in (k, n - k)] + [n // 2]
    for d in order:
        dest = (t + d) % n
        cols = pl.ds(pl.multiple_of((dest % h) * units, 128), units)
        for k in range(2):
            push(
                (gate, up)[k].at[rows, cols], w_block(t, first, part, k),
                w_send.at[d, k], w_recv.at[d, k], (g, dest, b),
            )

    for s in (2, 1) if square else range(1, h):
        dest = rows_of(j, s) if square else (j + s) % h
        push(tok.at[:, mine], T.at[j, :, mine], tok_send.at[s], tok_recv.at[s], (g, a * h + dest, b))
    push(down, D.at[b], d_send, d_recv, other)
    for load in loads:
        load.start()

    for d in order:
        source = (t + n - d) % n
        for k in range(2):
            block = w_block(source, first, part, k)
            remote(block, block, w_send.at[d, k], w_recv.at[d, k], other).wait_recv()
            for e in range(1, G):
                push(block, block, x_send.at[e, d, k], x_recv.at[e, d, k], ((g + e) % G, t, b))
    for load in loads:
        load.wait()
    remote(D.at[1 - b], D.at[1 - b], d_send, d_recv, other).wait_recv()
    total[...] = jnp.zeros_like(total)

    def tokens_arrive(s):
        block = token_block(s)
        remote(block, block, tok_send.at[s], tok_recv.at[s], other).wait_recv()
        if square and s < 3:
            @pl.when(b == s - 1)
            def _():
                target = flip2(j) if s == 1 else flip1(j)
                remote(block, block, tok_send.at[3], tok_recv.at[3], (g, a * h + target, b)).start()

        push(block, block, core_send.at[s], core_recv.at[s], other)

    def compute(s):
        slot = rows_of(j, s)
        if s > 0:
            block = T.at[slot, :, theirs]
            remote(block, block, core_send.at[s], core_recv.at[s], other).wait_recv()
        tiles = 4 if K % 512 == 0 else 1
        tile = K // tiles
        both[...] = jnp.zeros_like(both)

        def body(i, carry):
            k = pl.ds(pl.multiple_of(i * tile, 128), tile)
            both[...] += jnp.dot(T[slot, :, k], W[k, :], preferred_element_type=jnp.float32)
            return carry

        lax.fori_loop(0, tiles, body, 0)
        hidden = (jax.nn.silu(both[:, :units]) * both[:, units:]).astype(out.dtype)
        mine_h[s] = hidden

        @pl.when(a == b)
        def _():
            H[s, j, b] = hidden

        for d in sorted(range(1, pairs), key=lambda d: -min(d, pairs - d)):
            push(
                mine_h.at[s], H.at[s, j, b], h_send.at[s, d], h_recv.at[s, j // 2, b],
                (g, 2 * ((p + d) % pairs) + y, a),
            )

        @pl.when(a != b)
        def _():
            remote(mine_h.at[s], H.at[s, j, b], h_send.at[s, 0], h_recv.at[s, j // 2, b], other).start()

    def pass_on(s):
        for k in range(half):
            for c in range(B):
                block = H.at[s, 2 * k + y, c]

                @pl.when(jnp.logical_not((a == b) & (j // 2 == k) & (c == b)))
                def _():
                    remote(block, block, h_send.at[s, 0], h_recv.at[s, k, c], other).wait_recv()

                push(block, block, f_send.at[s, k, c], f_recv.at[s, k, c], across)

    def lower(s):
        for k in range(half):
            for c in range(B):
                block = H.at[s, 2 * k + 1 - y, c]
                remote(block, block, f_send.at[s, k, c], f_recv.at[s, k, c], across).wait_recv()

        def body(i, carry):
            r = rows_of(i, s)
            term = total[r]
            for c in range(B):
                term += jnp.dot(
                    H[s, i, c], D[c, pl.ds(pl.multiple_of(i * units, 128), units), :],
                    preferred_element_type=jnp.float32,
                )
            total[r] = term
            return carry

        lax.fori_loop(0, h, body, 0)

    for d in order:
        source = (t + n - d) % n
        for e in range(1, G):
            for k in range(2):
                block = w_block(source, ((g + G - e) % G) * part, part, k)
                remote(block, block, x_send.at[e, d, k], x_recv.at[e, d, k], other).wait_recv()

    compute(0)
    for s in range(1, h):
        tokens_arrive(s)
        compute(s)
        pass_on(s - 1)
        if s >= 2:
            lower(s - 2)
    pass_on(h - 1)
    lower(h - 2)
    lower(h - 1)
    for r in range(h):
        out[pl.ds(r * R, R), :] = total[r].astype(out.dtype)

    for c in pending:
        c.wait_send()
    if square:
        remote(token_block(1), token_block(1), tok_send.at[3], tok_recv.at[3], other).wait_send()

    @pl.when(a != b)
    def _():
        for s in range(h):
            remote(mine_h.at[s], mine_h.at[s], h_send.at[s, 0], h_recv.at[s, 0, 0], other).wait_send()


def local(G, n, B, tokens, gate_weight, up_weight, down_weight):
    h = n // B
    R, K = tokens.shape
    depth, wide = gate_weight.shape
    units, columns = wide // h, down_weight.shape[1]
    dtype = tokens.dtype
    DMA = pltpu.SemaphoreType.DMA
    return pl.pallas_call(
        functools.partial(layer, G, n, B),
        out_shape=jax.ShapeDtypeStruct((h * R, columns), dtype),
        in_specs=[ANY] * 4,
        out_specs=pl.BlockSpec(memory_space=pltpu.VMEM),
        scratch_shapes=[
            pltpu.VMEM((h, R, K), dtype),
            pltpu.VMEM((K, 2 * units), dtype),
            pltpu.VMEM((B, wide, columns), dtype),
            pltpu.VMEM((R, 2 * units), jnp.float32),
            pltpu.VMEM((h, R, units), dtype),
            pltpu.VMEM((h, h, B, R, units), dtype),
            pltpu.VMEM((h, R, columns), jnp.float32),
            DMA((4,)),
            DMA((h,)), DMA((h,)), DMA((h,)), DMA((h,)),
            DMA((n, 2)), DMA((n, 2)),
            DMA((G, n, 2)), DMA((G, n, 2)),
            DMA, DMA,
            DMA((h, n // 2)), DMA((h, h // 2, B)),
            DMA((h, h // 2, B)), DMA((h, h // 2, B)),
        ],
        compiler_params=pltpu.CompilerParams(
            collective_id=0, has_side_effects=True, vmem_limit_bytes=63_000_000
        ),
        name="layer",
    )(tokens, gate_weight, up_weight, down_weight)


def solution(mesh):
    shape = dict(mesh.shape)
    return jax.shard_map(
        functools.partial(local, shape["groups"], shape["tp"], shape["blk"]),
        mesh=mesh,
        in_specs=(P(("groups", "tp"), None), P("tp", "blk"), P("tp", "blk"), P("blk", "tp")),
        out_specs=P(("groups", "blk"), "tp"),
        check_vma=False,
    )
```

```python
import functools

import jax
import jax.numpy as jnp
from jax import lax
from jax.experimental import pallas as pl
from jax.experimental.pallas import tpu as pltpu
from jax.sharding import PartitionSpec as P

MESH = pl.DeviceIdType.MESH
ANY = pl.BlockSpec(memory_space=pl.ANY)


def flip1(i):
    return i + 1 - 2 * (i % 2)


def greet(devices):
    barrier = pltpu.get_barrier_semaphore()
    for device in devices:
        pl.semaphore_signal(barrier, inc=1, device_id=device, device_id_type=MESH)
    pl.semaphore_wait(barrier, len(devices))


def flip2(i):
    return i + 2 - 4 * ((i // 2) % 2)


CUT = 8


def layer(
    G, n, B,
    tok, gate, up, down, out,
    T, W, D, both, mine_h, H, total,
    lsem, tok_send, tok_recv, core_send, core_recv,
    w_send, w_recv, x_send, x_recv, d_send, d_recv,
    h_send, h_recv, f_send, f_recv,
):
    g, t, b = lax.axis_index("groups"), lax.axis_index("tp"), lax.axis_index("blk")
    h = n // B
    a, j = t // h, t % h
    half, pairs = h // 2, n // 2
    p, y = t // 2, t % 2
    other = (g, t, 1 - b)
    across = (g, flip1(t), b)
    R, K = tok.shape
    width = K // B
    depth, units = gate.shape[0], gate.shape[1] // h
    part = depth // G
    mine = pl.ds(pl.multiple_of(b * width, 128), width)
    theirs = pl.ds(pl.multiple_of((1 - b) * width, 128), width)
    square = h == 4
    cut = R * CUT // 16
    upper, lower_rows = pl.ds(0, cut), pl.ds(cut, R - cut)

    greet(
        [(g, (t + d) % n, b) for d in range(1, n)]
        + [(g, 2 * ((p + d) % pairs) + y, 1 - b) for d in range(1, pairs)]
        + [((g + e) % G, t, b) for e in range(1, G)]
        + [other]
    )

    def remote(src, dst, send, recv, device):
        return pltpu.make_async_remote_copy(
            src_ref=src, dst_ref=dst, send_sem=send, recv_sem=recv,
            device_id=device, device_id_type=MESH,
        )

    pending = []

    def push(*copy):
        c = remote(*copy)
        c.start()
        pending.append(c)

    def local(src, dst, sem):
        return pltpu.make_async_copy(src, dst, sem)

    def rows_of(i, s):
        if square:
            i = flip1(i) if s % 2 else i
            return flip2(i) if s // 2 else i
        return (i + h - s) % h

    def token_block(s):
        return T.at[rows_of(j, s), :, mine]

    def w_block(source, first, size, k):
        start = pl.multiple_of(source * depth + first, 16)
        return W.at[pl.ds(start, size), pl.ds(k * units, units)]

    own_columns = pl.ds(pl.multiple_of(j * units, 128), units)
    loads = [
        local(gate.at[:, own_columns], w_block(t, 0, depth, 0), lsem.at[0]),
        local(up.at[:, own_columns], w_block(t, 0, depth, 1), lsem.at[1]),
        local(tok, T.at[j], lsem.at[2]),
        local(down, D.at[b], lsem.at[3]),
    ]

    first = g * part
    rows = pl.ds(pl.multiple_of(first, 16), part)
    order = [d for k in range(1, n // 2) for d in (k, n - k)] + [n // 2]
    for d in order:
        dest = (t + d) % n
        cols = pl.ds(pl.multiple_of((dest % h) * units, 128), units)
        for k in range(2):
            push(
                (gate, up)[k].at[rows, cols], w_block(t, first, part, k),
                w_send.at[d, k], w_recv.at[d, k], (g, dest, b),
            )

    for s in (2, 1) if square else range(1, h):
        dest = rows_of(j, s) if square else (j + s) % h
        push(tok.at[:, mine], T.at[j, :, mine], tok_send.at[s], tok_recv.at[s], (g, a * h + dest, b))
    push(down, D.at[b], d_send, d_recv, other)
    for load in loads:
        load.start()

    for d in order:
        source = (t + n - d) % n
        for k in range(2):
            block = w_block(source, first, part, k)
            remote(block, block, w_send.at[d, k], w_recv.at[d, k], other).wait_recv()
            for e in range(1, G):
                push(block, block, x_send.at[e, d, k], x_recv.at[e, d, k], ((g + e) % G, t, b))
    for load in loads:
        load.wait()
    remote(D.at[1 - b], D.at[1 - b], d_send, d_recv, other).wait_recv()
    total[...] = jnp.zeros_like(total)

    def tokens_arrive(s):
        block = token_block(s)
        if square and s == 3:
            for i, r in ((3, upper), (0, lower_rows)):
                piece = T.at[rows_of(j, s), r, mine]
                remote(piece, piece, tok_send.at[i], tok_recv.at[i], other).wait_recv()
        else:
            remote(block, block, tok_send.at[s], tok_recv.at[s], other).wait_recv()
        if square and s < 3:
            piece = T.at[rows_of(j, s), (upper, lower_rows)[s - 1], mine]
            target = flip2(j) if s == 1 else flip1(j)
            i = 3 if s == 1 else 0
            push(piece, piece, tok_send.at[i], tok_recv.at[i], (g, a * h + target, b))

        push(block, block, core_send.at[s], core_recv.at[s], other)

    def compute(s):
        slot = rows_of(j, s)
        if s > 0:
            block = T.at[slot, :, theirs]
            remote(block, block, core_send.at[s], core_recv.at[s], other).wait_recv()
        tiles = 4 if K % 512 == 0 else 1
        tile = K // tiles
        both[...] = jnp.zeros_like(both)

        def body(i, carry):
            k = pl.ds(pl.multiple_of(i * tile, 128), tile)
            both[...] += jnp.dot(T[slot, :, k], W[k, :], preferred_element_type=jnp.float32)
            return carry

        lax.fori_loop(0, tiles, body, 0)
        hidden = (jax.nn.silu(both[:, :units]) * both[:, units:]).astype(out.dtype)
        mine_h[s] = hidden

        @pl.when(a == b)
        def _():
            H[s, j, b] = hidden

        for d in sorted(range(1, pairs), key=lambda d: min(d, pairs - d)):
            push(
                mine_h.at[s], H.at[s, j, b], h_send.at[s, d], h_recv.at[s, j // 2, b],
                (g, 2 * ((p + d) % pairs) + y, a),
            )

        @pl.when(a != b)
        def _():
            remote(mine_h.at[s], H.at[s, j, b], h_send.at[s, 0], h_recv.at[s, j // 2, b], other).start()

    def pass_on(s):
        for k in range(half):
            for c in range(B):
                block = H.at[s, 2 * k + y, c]

                @pl.when(jnp.logical_not((a == b) & (j // 2 == k) & (c == b)))
                def _():
                    remote(block, block, h_send.at[s, 0], h_recv.at[s, k, c], other).wait_recv()

                push(block, block, f_send.at[s, k, c], f_recv.at[s, k, c], across)

    def lower(s):
        for k in range(half):
            for c in range(B):
                block = H.at[s, 2 * k + 1 - y, c]
                remote(block, block, f_send.at[s, k, c], f_recv.at[s, k, c], across).wait_recv()

        def body(i, carry):
            r = rows_of(i, s)
            term = total[r]
            for c in range(B):
                term += jnp.dot(
                    H[s, i, c], D[c, pl.ds(pl.multiple_of(i * units, 128), units), :],
                    preferred_element_type=jnp.float32,
                )
            total[r] = term
            return carry

        lax.fori_loop(0, h, body, 0)

    for d in order:
        source = (t + n - d) % n
        for e in range(1, G):
            for k in range(2):
                block = w_block(source, ((g + G - e) % G) * part, part, k)
                remote(block, block, x_send.at[e, d, k], x_recv.at[e, d, k], other).wait_recv()

    compute(0)
    for s in range(1, h):
        tokens_arrive(s)
        compute(s)
        pass_on(s - 1)
        if s >= 2:
            lower(s - 2)
    pass_on(h - 1)
    lower(h - 2)
    lower(h - 1)
    for r in range(h):
        out[pl.ds(r * R, R), :] = total[r].astype(out.dtype)

    for c in pending:
        c.wait_send()
    @pl.when(a != b)
    def _():
        for s in range(h):
            remote(mine_h.at[s], mine_h.at[s], h_send.at[s, 0], h_recv.at[s, 0, 0], other).wait_send()


def local(G, n, B, tokens, gate_weight, up_weight, down_weight):
    h = n // B
    R, K = tokens.shape
    depth, wide = gate_weight.shape
    units, columns = wide // h, down_weight.shape[1]
    dtype = tokens.dtype
    DMA = pltpu.SemaphoreType.DMA
    return pl.pallas_call(
        functools.partial(layer, G, n, B),
        out_shape=jax.ShapeDtypeStruct((h * R, columns), dtype),
        in_specs=[ANY] * 4,
        out_specs=pl.BlockSpec(memory_space=pltpu.VMEM),
        scratch_shapes=[
            pltpu.VMEM((h, R, K), dtype),
            pltpu.VMEM((K, 2 * units), dtype),
            pltpu.VMEM((B, wide, columns), dtype),
            pltpu.VMEM((R, 2 * units), jnp.float32),
            pltpu.VMEM((h, R, units), dtype),
            pltpu.VMEM((h, h, B, R, units), dtype),
            pltpu.VMEM((h, R, columns), jnp.float32),
            DMA((4,)),
            DMA((h,)), DMA((h,)), DMA((h,)), DMA((h,)),
            DMA((n, 2)), DMA((n, 2)),
            DMA((G, n, 2)), DMA((G, n, 2)),
            DMA, DMA,
            DMA((h, n // 2)), DMA((h, h // 2, B)),
            DMA((h, h // 2, B)), DMA((h, h // 2, B)),
        ],
        compiler_params=pltpu.CompilerParams(
            collective_id=0, has_side_effects=True, vmem_limit_bytes=63_000_000
        ),
        name="layer",
    )(tokens, gate_weight, up_weight, down_weight)


def solution(mesh):
    shape = dict(mesh.shape)
    return jax.shard_map(
        functools.partial(local, shape["groups"], shape["tp"], shape["blk"]),
        mesh=mesh,
        in_specs=(P(("groups", "tp"), None), P("tp", "blk"), P("tp", "blk"), P("blk", "tp")),
        out_specs=P(("groups", "blk"), "tp"),
        check_vma=False,
    )
```
